32 devices in a mesh: group: 4 (over z), shard: 8 (over y, x, core).
Axes of the slice: x: 2, y: 2, z: 4, core: 2. Of those that a mesh axis runs over, the one named last changes fastest.
Arguments:
- hidden_state: bfloat16 [512, 8192], P('group', 'shard'), may hold values from -40 to 40
- attn_gain: bfloat16 [8192], replicated, may hold values from 0.5 to 1.5
- ffn_gain: bfloat16 [8192], replicated, may hold values from 0.5 to 1.5
- w_query: bfloat16 [8192, 8192], P('group', 'shard'), may hold values from -0.125 to 0.125
- w_keyval: bfloat16 [8192, 2048], P('group', 'shard'), may hold values from -0.0625 to 0.0625
- w_output: bfloat16 [8192, 8192], P('shard', 'group'), may hold values from -0.0625 to 0.0625
- cache_keys: bfloat16 [512, 8, 192, 128], P(('group', 'shard')), may hold values from -256 to 256
- cache_values: bfloat16 [512, 8, 192, 128], P(('group', 'shard')), may hold values from -6 to 6
- lengths: int32 [512], P('group'), may hold values from 2 to 192, as said below
Outputs:
- branch: bfloat16 [512, 8192], P('group', 'shard')
- ffn_input: bfloat16 [512, 8192], P('group', 'shard')
The draws below stay inside these ranges and needn't reach their ends.
Inputs may be any that keep to these rules, and one draw needn't show every extreme that they name: `lengths`: in every aligned block of 16 sequences, at least one has all 192 cached positions live.
All inputs are finite; a program needn't handle non-finite values.
Results may differ from the reference program's by a relative error of at most 0.012.
The reference program's roundings to bfloat16 on the way count: a program that leaves them out, or rounds other values in their place, can miss the bound.
Values may be sent and summed in bfloat16 or wider, within the bound.
A program may use at most 128 MiB of HBM per device.

```python
import jax
import jax.numpy as jnp
from jax import lax

D = 8192
HEADS = 64
KVH = 8
HD = 128
SEQ_DEV = 16
CACHE = 192
SEQS = 512


def draw_hidden_state(key, part):
    rows_key, cols_key, noise_key = jax.random.split(key, 3)
    position = jnp.arange(D, dtype=jnp.float32) / D
    column_scale = 0.3 * 10.0 ** (0.5 * position + 0.5 * jax.random.uniform(cols_key, (D,), dtype=jnp.float32))
    row_scale = 10.0 ** jax.random.uniform(rows_key, (SEQS, 1), dtype=jnp.float32, minval=-0.5, maxval=0.5)
    values = jax.random.normal(noise_key, (SEQS, D), dtype=jnp.float32) * column_scale[None, :] * row_scale
    return jnp.clip(values, -40.0, 40.0).astype(jnp.bfloat16)


def draw_cache_keys(key, part):
    base_key = jax.random.fold_in(jax.random.fold_in(key, 17), 0)
    shape = (SEQS, KVH, CACHE, HD)
    values = jax.random.normal(base_key, shape, dtype=jnp.float32)
    return jnp.clip(values, -256.0, 256.0).astype(jnp.bfloat16)


def draw_lengths(key, part):
    fill_key, pick_key = jax.random.split(jax.random.fold_in(key, 29))
    drawn = jax.random.randint(fill_key, (SEQS,), 2, CACHE + 1)
    chosen = jax.random.randint(pick_key, (SEQS // SEQ_DEV, 1), 0, SEQ_DEV)
    full_row = (jnp.arange(SEQ_DEV, dtype=jnp.int32)[None, :] == chosen).reshape(SEQS)
    return jnp.where(full_row, CACHE, drawn).astype(jnp.int32)


def shard_levels(own_key, dims, cuts, smallest, high):
    loudness = 1.0
    for axis_at, shards_of in cuts:
        steps = jax.random.uniform(jax.random.fold_in(jax.random.fold_in(own_key, 6), axis_at), (shards_of,), jnp.float32, smallest / len(cuts), high / len(cuts))
        loudness = loudness * jnp.repeat(jnp.exp(steps), dims[axis_at] // shards_of).reshape((-1,) + (1,) * (len(dims) - 1 - axis_at))
    return loudness


def centred(key, extent, scale, limit, cuts=(), held_as=jnp.bfloat16):
    loudness = shard_levels(key, extent, cuts, -0.22, 0.18) if cuts else 1.0
    values = jax.random.normal(key, extent, jnp.float32) * scale * loudness
    return jnp.minimum(jnp.maximum(values, -limit), limit).astype(held_as)


def setup_inputs(seed: int = 0) -> dict:
    arg_keys = jax.random.split(jax.random.key(seed), 10)
    hidden_state = draw_hidden_state(jax.random.fold_in(arg_keys[9], 71), 0)
    attn_gain = jnp.clip(1.0 + 0.1 * jax.random.normal(arg_keys[1], (D,), jnp.float32), 0.5, 1.5).astype(jnp.bfloat16)
    ffn_gain = jnp.clip(1.0 + 0.1 * jax.random.normal(arg_keys[2], (D,), jnp.float32), 0.5, 1.5).astype(jnp.bfloat16)
    w_query = centred(arg_keys[3], (D, HEADS * HD), (D // 4) ** -0.5, 0.125, ((0, 4), (1, 8)))
    w_keyval = centred(arg_keys[4], (D, 2 * KVH * HD), D ** -0.5, 0.0625, ((0, 4), (1, 8)))
    w_output = centred(arg_keys[5], (HEADS * HD, D), (HEADS * HD) ** -0.5, 0.0625, ((0, 8), (1, 4)))
    cache_keys = draw_cache_keys(jax.random.fold_in(arg_keys[9], 71), 0)
    cache_values = centred(arg_keys[7], (SEQS, KVH, CACHE, HD), 1.0, 6.0, ((0, 32),))
    lengths = draw_lengths(jax.random.fold_in(arg_keys[9], 71), 0)
    return dict(hidden_state=hidden_state, attn_gain=attn_gain, ffn_gain=ffn_gain, w_query=w_query, w_keyval=w_keyval, w_output=w_output, cache_keys=cache_keys, cache_values=cache_values, lengths=lengths)


epsilon = 1e-05
rope_base = 500000.0

def rotate(heads_block, position):
    head_dim = heads_block.shape[-1]
    half_dim = head_dim // 2
    frequency = rope_base ** (-2.0 * jnp.arange(half_dim, dtype=jnp.float32) / head_dim)
    angles = position.astype(jnp.float32)[:, None] * frequency[None, :]
    cosine = jnp.cos(angles)[:, None, :]
    sine_part = jnp.sin(angles)[:, None, :]
    lower_half = heads_block[..., :half_dim]
    upper_half = heads_block[..., half_dim:]
    return jnp.concatenate([lower_half * cosine - upper_half * sine_part, upper_half * cosine + lower_half * sine_part], axis=-1)

def attend(queries, fresh, cache_keys, cache_values, lengths):
    seq_count, kv_heads, cache_len, head_dim = cache_keys.shape
    q_heads = queries.shape[1] // head_dim
    q_per_kv = q_heads // kv_heads
    kv_width = kv_heads * head_dim
    grouped = queries.astype(jnp.float32).reshape(seq_count, kv_heads, q_per_kv, head_dim)
    new_keys = fresh[:, :kv_width].astype(jnp.float32).reshape(seq_count, kv_heads, head_dim)
    new_values = fresh[:, kv_width:].astype(jnp.float32).reshape(seq_count, kv_heads, head_dim)
    score_scale = head_dim ** (-0.5)
    scores = jnp.einsum('nkgd,nkld->nkgl', grouped, cache_keys.astype(jnp.float32)) * score_scale
    self_score = jnp.einsum('nkgd,nkd->nkg', grouped, new_keys) * score_scale
    live_mask = jnp.arange(cache_len, dtype=jnp.int32)[None, :] < lengths[:, None]
    scores = jnp.where(live_mask[:, None, None, :], scores, -1e+30)
    row_top = jnp.maximum(lax.optimization_barrier(jnp.max(scores, axis=3)), self_score)
    exp_scores = jnp.exp(scores - row_top[..., None])
    self_weight = jnp.exp(self_score - row_top)
    denom_sum = lax.optimization_barrier(jnp.sum(exp_scores, axis=3)) + self_weight
    weight_bf = (exp_scores / denom_sum[..., None]).astype(jnp.bfloat16)
    self_bf = (self_weight / denom_sum).astype(jnp.bfloat16)
    context = jnp.einsum('nkgl,nkld->nkgd', weight_bf.astype(jnp.float32), cache_values.astype(jnp.float32))
    context = context + self_bf.astype(jnp.float32)[..., None] * new_values[:, :, None, :]
    return context.reshape(seq_count, q_heads * head_dim).astype(jnp.bfloat16)

def reference(hidden_state, attn_gain, ffn_gain, w_query, w_keyval, w_output, cache_keys, cache_values, lengths):
    resident = hidden_state.astype(jnp.float32)
    inverse = lax.rsqrt(lax.optimization_barrier(jnp.mean(resident * resident, axis=1, keepdims=True)) + epsilon)
    normed = (resident * inverse * attn_gain.astype(jnp.float32)).astype(jnp.bfloat16)
    queries = jnp.dot(normed, w_query, preferred_element_type=jnp.float32)
    keyval = jnp.dot(normed, w_keyval, preferred_element_type=jnp.float32)
    seq_total = queries.shape[0]
    kv_width = KVH * HD
    roped_q = rotate(queries.reshape(seq_total, HEADS, HD), lengths).reshape(seq_total, HEADS * HD).astype(jnp.bfloat16)
    new_keys = rotate(keyval[:, :kv_width].reshape(seq_total, KVH, HD), lengths).reshape(seq_total, kv_width).astype(jnp.bfloat16)
    new_values = keyval[:, kv_width:].astype(jnp.bfloat16)
    fresh = jnp.concatenate([new_keys, new_values], axis=1)
    block_count = seq_total // SEQ_DEV

    def one_block(pieces):
        return attend(pieces[0], pieces[1], pieces[2], pieces[3], pieces[4])
    contexts = lax.map(one_block, (roped_q.reshape(block_count, SEQ_DEV, HEADS * HD), fresh.reshape(block_count, SEQ_DEV, 2 * kv_width), cache_keys.reshape(block_count, SEQ_DEV, KVH, CACHE, HD), cache_values.reshape(block_count, SEQ_DEV, KVH, CACHE, HD), lengths.reshape(block_count, SEQ_DEV)))
    context = contexts.reshape(seq_total, HEADS * HD)
    summed = jnp.dot(context, w_output, preferred_element_type=jnp.float32)
    branch = summed.astype(jnp.bfloat16)
    stream = resident + summed
    inverse_two = lax.rsqrt(lax.optimization_barrier(jnp.mean(stream * stream, axis=1, keepdims=True)) + epsilon)
    ffn_input = (stream * inverse_two * ffn_gain.astype(jnp.float32)).astype(jnp.bfloat16)
    return (branch, ffn_input)
```

```python
import functools
import math

import jax
import jax.numpy as jnp
from jax import lax
from jax.experimental import pallas as pl
from jax.experimental.pallas import tpu as pltpu
from jax.sharding import PartitionSpec as P

epsilon = 1e-05
rope_base = 500000.0
MESH = pl.DeviceIdType.MESH
VMEM = pl.BlockSpec(memory_space=pltpu.VMEM)
BF = jnp.bfloat16
F32 = jnp.float32


def device(group, shard):
    return {"group": group, "shard": shard}


def partner_of(k, sizes, sign=1):
    groups, shards = sizes
    g, s = lax.axis_index("group"), lax.axis_index("shard")
    dg, ds = k // shards, k % shards
    if sign > 0:
        return lax.rem(g + dg, groups), lax.rem(s + ds, shards)
    return lax.rem(g - dg + groups, groups), lax.rem(s - ds + shards, shards)


def greet(sizes, total):
    barrier = pltpu.get_barrier_semaphore()

    def signal(k, carry):
        pl.semaphore_signal(
            barrier, inc=1, device_id=device(*partner_of(k, sizes)), device_id_type=MESH
        )
        return carry

    lax.fori_loop(1, total, signal, 0)
    pl.semaphore_wait(barrier, total - 1)


def remote(src, dst, send, recv, where):
    return pltpu.make_async_remote_copy(
        src_ref=src,
        dst_ref=dst,
        send_sem=send,
        recv_sem=recv,
        device_id=device(*where),
        device_id_type=MESH,
    )


def exchange_kernel(sizes, total, src_at, dst_at, count, *refs):
    ins, outs = refs[:count], refs[count : 2 * count]
    sends, recvs, own = refs[2 * count :]
    g, s = lax.axis_index("group"), lax.axis_index("shard")
    locals_ = [
        pltpu.make_async_copy(src_at(a, g, s), dst_at(b, g, s), own.at[i])
        for i, (a, b) in enumerate(zip(ins, outs))
    ]
    for c in locals_:
        c.start()
    greet(sizes, total)

    def start(j, carry):
        k = lax.rem(j, sizes[0]) * sizes[1] + j // sizes[0]
        pg, ps = partner_of(k, sizes)
        for i in range(count):
            remote(
                src_at(ins[i], pg, ps),
                dst_at(outs[i], g, s),
                sends.at[i, k],
                recvs.at[i, k],
                (pg, ps),
            ).start()
        return carry

    lax.fori_loop(1, total, start, 0)

    def finish(j, carry):
        k = lax.rem(j, sizes[0]) * sizes[1] + j // sizes[0]
        pg, ps = partner_of(k, sizes)
        fg, fs = partner_of(k, sizes, -1)
        for i in range(count):
            copy = remote(
                src_at(ins[i], pg, ps),
                dst_at(outs[i], fg, fs),
                sends.at[i, k],
                recvs.at[i, k],
                (pg, ps),
            )
            copy.wait_send()
            copy.wait_recv()
        return carry

    lax.fori_loop(1, total, finish, 0)
    for c in locals_:
        c.wait()


def exchange(arrays, outs, sizes, total, src_at, dst_at, ident):
    count = len(arrays)
    return pl.pallas_call(
        functools.partial(exchange_kernel, sizes, total, src_at, dst_at, count),
        out_shape=[jax.ShapeDtypeStruct(o, a.dtype) for o, a in zip(outs, arrays)],
        in_specs=[VMEM] * count,
        out_specs=[VMEM] * count,
        scratch_shapes=[
            pltpu.SemaphoreType.DMA((count, total)),
            pltpu.SemaphoreType.DMA((count, total)),
            pltpu.SemaphoreType.DMA((count,)),
        ],
        compiler_params=pltpu.CompilerParams(collective_id=ident, has_side_effects=True),
    )(*arrays)


pieces = 4
lanes = 128


def near(sizes):
    groups, shards = sizes
    g, s = lax.axis_index("group"), lax.axis_index("shard")
    out = [(g, lax.rem(s + d, shards)) for d in range(1, shards)]
    return out + [(lax.rem(g + d, groups), s) for d in range(1, groups)]


def meet(sizes):
    barrier = pltpu.get_barrier_semaphore()
    partners = near(sizes)
    for where in partners:
        pl.semaphore_signal(barrier, inc=1, device_id=device(*where), device_id_type=MESH)
    pl.semaphore_wait(barrier, len(partners))


def turn(j, g, groups):
    up, down = groups - 1 - g, g
    both = jnp.minimum(up, down)
    paired = jnp.where(lax.rem(j, 2) == 0, groups - 1 - j // 2, j // 2)
    rest = jnp.where(up > down, groups - 1 - (j - both), j - both)
    return jnp.where(j < 2 * both, paired, jnp.where(j == groups - 1, g, rest))


def wait_for(dst, sem):
    pltpu.make_async_copy(dst, dst, sem).wait()


def front_kernel(
    sizes,
    x_ref,
    gain_ref,
    pos_ref,
    freq_ref,
    wq_ref,
    wkv_ref,
    got_ref,
    stage,
    block,
    ss,
    sums,
    totals,
    weight,
    normed,
    inbuf,
    outbuf,
    fin,
    cosines,
    sines,
    load,
    own,
    s1,
    r1,
    s2,
    r2,
    s3,
    r3,
    s4,
    r4,
    sp,
    rp,
    sg,
    rg,
    s5,
    r5,
    s6,
    r6,
):
    groups, shards = sizes
    chips = shards // 2
    span, width = x_ref.shape[1:]
    tokens = span * chips
    seqs = tokens // shards
    depth = weight.shape[0]
    q_cols = wq_ref.shape[1]
    blocks, _, _, wide = fin.shape
    g, s = lax.axis_index("group"), lax.axis_index("shard")
    chip, core = s // 2, lax.rem(s, 2)
    sibling = chip * 2 + 1 - core
    loads = [
        pltpu.make_async_copy(wq_ref, weight.at[:, pl.ds(0, q_cols)], load.at[0]),
        pltpu.make_async_copy(
            wkv_ref, weight.at[:, pl.ds(q_cols, wkv_ref.shape[1])], load.at[1]
        ),
    ]
    for c in loads:
        c.start()
    meet(sizes)

    def half(which):
        return pl.ds(pl.multiple_of(which * width, width), width)

    def scatter(d):
        t = lax.rem(chip + d, chips)
        return remote(x_ref.at[t], stage.at[chip], s1.at[d], r1.at[chip], (g, t * 2 + core))

    for d in range(1, chips):
        scatter(d).start()

    part = jnp.zeros((tokens, lanes), F32)
    for j in range(width // lanes):
        v = x_ref[:, :, j * lanes : (j + 1) * lanes].reshape(tokens, lanes).astype(F32)
        part = part + v * v
    ss[...] = jnp.sum(part.T, axis=0, keepdims=True)
    sums[s] = ss[...]

    def plane_sum(d, slot):
        return remote(ss, sums.at[slot], sp.at[d], rp.at[d], (g, lax.rem(s + d, shards)))

    for d in range(1, shards):
        plane_sum(d, s).start()

    def lift(c, src):
        return remote(src, block.at[g, chip, :, half(core)], s2.at[c], r2.at[g], (c, s))

    def pass_on(j, carry):
        c = turn(j, g, groups)

        @pl.when(c != chip)
        def _():
            wait_for(stage.at[c], r1.at[c])

        @pl.when((c != g) & (c != chip))
        def _():
            lift(c, stage.at[c]).start()

        @pl.when((c != g) & (c == chip))
        def _():
            lift(c, x_ref.at[c]).start()

        dst = block.at[g, chip, :, half(core)]

        @pl.when((c == g) & (c != chip))
        def _():
            pltpu.make_async_copy(stage.at[c], dst, r2.at[g]).start()

        @pl.when((c == g) & (c == chip))
        def _():
            pltpu.make_async_copy(x_ref.at[c], dst, r2.at[g]).start()

        return carry

    lax.fori_loop(0, groups, pass_on, 0)

    for d in range(1, shards):
        plane_sum(d, lax.rem(s - d + shards, shards)).wait_recv()
    total = sums[0]
    for t in range(1, shards):
        total = total + sums[t]
    totals[g] = total

    def group_sum(d, slot):
        return remote(
            totals.at[g], totals.at[slot], sg.at[d], rg.at[d], (lax.rem(g + d, groups), s)
        )

    for d in range(1, groups):
        group_sum(d, g).start()

    def ring(p, c):
        ref = block.at[p, chip, :, half(core)]
        to = lax.rem(chip + c, chips) * 2 + core
        return remote(ref, ref, s3.at[p, c], r3.at[p, c], (g, to))

    def ring_at(p, c, which):
        return block.at[p, lax.rem(chip + chips - c, chips), :, half(which)]

    def pair(p, c):
        ref = ring_at(p, c, core)
        return remote(ref, ref, s4.at[p, c], r4.at[p, c], (g, sibling))

    def share(j, carry):
        p = turn(j, g, groups)
        wait_for(block.at[p, chip, :, half(core)], r2.at[p])
        for c in range(1, chips):
            ring(p, c).start()
        pair(p, 0).start()
        return carry

    lax.fori_loop(0, groups, share, 0)

    position = jnp.broadcast_to(pos_ref[...].astype(F32), (lanes, tokens)).T
    angle = position * freq_ref[...]
    low = lax.broadcasted_iota(jnp.int32, (tokens, lanes), 1) < lanes // 2
    cosines[...] = jnp.cos(angle)
    sine = jnp.sin(angle)
    sines[...] = jnp.where(low, -sine, sine)

    for d in range(1, groups):
        group_sum(d, lax.rem(g - d + groups, groups)).wait_recv()
    for c in loads:
        c.wait()

    def slot_of(p, to, frm):
        return jnp.where((p == to) & (frm > to), groups, p)

    def send(p, n):
        to = jnp.where(p > g, g + 1, g - 1)
        slot = slot_of(p, to, g)
        return remote(outbuf.at[p, n], inbuf.at[slot, n], s5.at[p, n], r5.at[slot, n], (to, s))

    def product(n):
        return jnp.dot(
            normed[...],
            weight[:, pl.ds(pl.multiple_of(n * wide, wide), wide)],
            preferred_element_type=F32,
        )

    def prepare(p):
        for c in range(1, chips):
            wait_for(ring_at(p, c, core), r3.at[p, c])
            pair(p, c).start()
        for c in range(chips):
            wait_for(ring_at(p, c, 1 - core), r4.at[p, c])
        inverse = lax.rsqrt(totals[p] / (depth * groups) + epsilon)
        inverse = jnp.broadcast_to(inverse, (lanes, tokens)).T
        for j in range(depth // lanes):
            cols = pl.ds(j * lanes, lanes)
            v = block[p, :, :, cols].reshape(tokens, lanes).astype(F32)
            normed[:, cols] = (v * inverse * gain_ref[:, cols]).astype(BF)

    def reduce(j, carry):
        p = turn(j, g, groups)
        prepare(p)
        fed = jnp.where(p > g, g > 0, g < groups - 1)

        def columns(n, carry):
            outbuf[p, n] = product(n).astype(BF)

            @pl.when(fed)
            def _():
                wait_for(inbuf.at[p, n], r5.at[p, n])
                outbuf[p, n] = (outbuf[p, n].astype(F32) + inbuf[p, n].astype(F32)).astype(BF)

            send(p, n).start()
            return carry

        lax.fori_loop(0, blocks, columns, 0)
        return carry

    lax.fori_loop(0, groups - 1, reduce, 0)
    prepare(g)
    is_key = s < shards // 2

    def deliver(n, d, slot):
        t = lax.rem(s + d, shards)
        return remote(fin.at[n, t], got_ref.at[slot, n], s6.at[n, d], r6.at[n, d], (g, t))

    def finish_own(n, carry):
        acc = product(n)
        above = jnp.where(g > 0, 1.0, 0.0)
        below = jnp.where(g < groups - 1, 1.0, 0.0)

        @pl.when(g == 0)
        def _():
            inbuf[g, n] = jnp.zeros_like(inbuf[g, n])

        @pl.when(g == groups - 1)
        def _():
            inbuf[groups, n] = jnp.zeros_like(inbuf[groups, n])

        @pl.when(g > 0)
        def _():
            wait_for(inbuf.at[g, n], r5.at[g, n])

        @pl.when(g < groups - 1)
        def _():
            wait_for(inbuf.at[groups, n], r5.at[groups, n])

        acc = acc + inbuf[g, n].astype(F32) + inbuf[groups, n].astype(F32)
        turned = is_key | (n * wide < q_cols)
        cosine = jnp.where(turned, cosines[...], 1.0)
        sine = jnp.where(turned, sines[...], 0.0)
        for h in range(wide // lanes):
            v = acc[:, h * lanes : (h + 1) * lanes]
            v = v * cosine + pltpu.roll(v, lanes // 2, 1) * sine
            fin[n, :, :, pl.ds(h * lanes, lanes)] = v.reshape(shards, seqs, lanes).astype(BF)
        got_ref[s, n] = fin[n, s]
        for d in range(1, shards):
            deliver(n, d, s).start()
        return carry

    lax.fori_loop(0, blocks, finish_own, 0)

    def settle(n, carry):
        for d in range(1, shards):
            deliver(n, d, lax.rem(s - d + shards, shards)).wait()
        return carry

    lax.fori_loop(0, blocks, settle, 0)

    def drain(j, carry):
        p = turn(j, g, groups)

        def each(n, carry):
            send(p, n).wait_send()
            return carry

        lax.fori_loop(0, blocks, each, 0)
        return carry

    lax.fori_loop(0, groups - 1, drain, 0)
    for d in range(1, chips):
        scatter(d).wait_send()
    for d in range(1, shards):
        plane_sum(d, s).wait_send()
    for d in range(1, groups):
        group_sum(d, g).wait_send()

    def drain_block(p, carry):
        @pl.when(p != g)
        def _():
            lift(p, x_ref.at[p]).wait_send()

        pair(p, 0).wait_send()
        for c in range(1, chips):
            ring(p, c).wait_send()
            pair(p, c).wait_send()
        return carry

    lax.fori_loop(0, groups, drain_block, 0)


def front(x, gain, positions, frequencies, w_query, w_keyval, sizes):
    groups, shards = sizes
    chips = shards // 2
    tokens, width = x.shape
    span = tokens // chips
    seqs = tokens // shards
    depth = w_query.shape[0]
    cols = w_query.shape[1] + w_keyval.shape[1]
    wide = math.gcd(cols, 256)
    wide = math.gcd(wide, w_query.shape[1])
    blocks = cols // wide
    dma = pltpu.SemaphoreType.DMA
    hbm = pl.BlockSpec(memory_space=pl.ANY)
    return pl.pallas_call(
        functools.partial(front_kernel, sizes),
        out_shape=jax.ShapeDtypeStruct((shards, blocks, seqs, wide), BF),
        in_specs=[VMEM] * 4 + [hbm] * 2,
        out_specs=VMEM,
        scratch_shapes=[
            pltpu.VMEM((chips, span, width), BF),
            pltpu.VMEM((groups, chips, span, depth), BF),
            pltpu.VMEM((1, tokens), F32),
            pltpu.VMEM((shards, 1, tokens), F32),
            pltpu.VMEM((groups, 1, tokens), F32),
            pltpu.VMEM((depth, cols), BF),
            pltpu.VMEM((tokens, depth), BF),
            pltpu.VMEM((groups + 1, blocks, tokens, wide), BF),
            pltpu.VMEM((groups, blocks, tokens, wide), BF),
            pltpu.VMEM((blocks, shards, seqs, wide), BF),
            pltpu.VMEM((tokens, lanes), F32),
            pltpu.VMEM((tokens, lanes), F32),
            dma((2,)),
            dma((1,)),
            dma((chips,)),
            dma((chips,)),
            dma((groups,)),
            dma((groups,)),
            dma((groups, chips)),
            dma((groups, chips)),
            dma((groups, chips)),
            dma((groups, chips)),
            dma((shards,)),
            dma((shards,)),
            dma((groups,)),
            dma((groups,)),
            dma((groups, blocks)),
            dma((groups + 1, blocks)),
            dma((blocks, shards)),
            dma((blocks, shards)),
        ],
        compiler_params=pltpu.CompilerParams(collective_id=1, has_side_effects=True),
    )(x.reshape(chips, span, width), gain, positions, frequencies, w_query, w_keyval)


def finish_kernel(
    sizes,
    p_ref,
    x_ref,
    gain_ref,
    branch_ref,
    ffn_ref,
    sib,
    mid,
    got,
    total_ref,
    fin,
    squares,
    s0,
    r0,
    s1,
    r1,
    s2,
    r2,
    s3,
    r3,
):
    groups, shards = sizes
    chips = shards // 2
    tokens, width = x_ref.shape
    model = width * shards
    g, s = lax.axis_index("group"), lax.axis_index("shard")
    chip, core = s // 2, lax.rem(s, 2)
    sibling = chip * 2 + 1 - core
    greet(sizes, groups * shards)
    order = list(range(1, chips)) + [0]
    span = tokens // pieces

    def block(c):
        return lax.rem(chip + c, chips)

    def half(which):
        return pl.ds(pl.multiple_of(which * width, width), width)

    def rows(q):
        return pl.ds(q * span, span)

    def near(q, c):
        a = block(c)
        return remote(
            p_ref.at[a, rows(q), half(1 - core)],
            sib.at[a, rows(q)],
            s0.at[q, c],
            r0.at[q, c],
            (g, sibling),
        )

    def far(q, c):
        a = block(c)
        return remote(
            mid.at[a, rows(q)],
            got.at[c, rows(q)],
            s1.at[q, c],
            r1.at[q, c],
            (g, a * 2 + core),
        )

    def swap(q):
        return remote(
            total_ref.at[rows(q)], fin.at[rows(q)], s2.at[q], r2.at[q], (chip, g * 2 + core)
        )

    for q in range(pieces):
        for c in order:
            near(q, c).start()
    for q in range(pieces):
        for c in order:
            a = block(c)
            near(q, c).wait_recv()
            mid[a, rows(q)] = (
                p_ref[a, rows(q), half(core)].astype(F32) + sib[a, rows(q)].astype(F32)
            ).astype(BF)
            if c:
                far(q, c).start()
    for q in range(pieces):
        acc = mid[chip, rows(q)].astype(F32)
        for c in order[:-1]:
            far(q, c).wait_recv()
            acc = acc + got[c, rows(q)].astype(F32)
        total_ref[rows(q)] = acc.astype(BF)

        @pl.when(chip != g)
        def _():
            swap(q).start()

        @pl.when(chip == g)
        def _():
            pltpu.make_async_copy(total_ref.at[rows(q)], fin.at[rows(q)], r2.at[q]).start()

    parts = []
    for q in range(pieces):
        pltpu.make_async_copy(fin.at[rows(q)], fin.at[rows(q)], r2.at[q]).wait()
        branch_ref[rows(q)] = fin[rows(q)]
        part = jnp.zeros((span, lanes), F32)
        for j in range(width // lanes):
            cols = pl.ds(j * lanes, lanes)
            stream = x_ref[rows(q), cols].astype(F32) + fin[rows(q), cols].astype(F32)
            part = part + stream * stream
        parts.append(part)
    flipped = jnp.concatenate(parts, axis=0).T
    squares[s] = jnp.sum(flipped, axis=0, keepdims=True)

    def tell(ds, slot):
        to = lax.rem(s + ds, shards)
        return remote(squares.at[slot], squares.at[slot], s3.at[ds], r3.at[ds], (g, to))

    for ds in range(1, shards):
        tell(ds, s).start()
    for q in range(pieces):
        for c in order:
            near(q, c).wait_send()
            if c:
                far(q, c).wait_send()

        @pl.when(chip != g)
        def _():
            swap(q).wait_send()

    for ds in range(1, shards):
        tell(ds, lax.rem(s - ds + shards, shards)).wait_recv()
    square_sum = squares[0]
    for t in range(1, shards):
        square_sum = square_sum + squares[t]
    inverse = lax.rsqrt(square_sum / model + epsilon)
    inverse = jnp.broadcast_to(inverse, (lanes, tokens)).T
    for j in range(width // lanes):
        cols = pl.ds(j * lanes, lanes)
        stream = x_ref[:, cols].astype(F32) + fin[:, cols].astype(F32)
        ffn_ref[:, cols] = (stream * inverse * gain_ref[:, cols]).astype(BF)
    for ds in range(1, shards):
        tell(ds, s).wait_send()


def finish(partial, x, gain, sizes):
    groups, shards = sizes
    chips = shards // 2
    tokens, width = x.shape
    dma = pltpu.SemaphoreType.DMA
    return pl.pallas_call(
        functools.partial(finish_kernel, sizes),
        out_shape=[jax.ShapeDtypeStruct((tokens, width), BF)] * 2,
        in_specs=[VMEM] * 3,
        out_specs=[VMEM] * 2,
        scratch_shapes=[
            pltpu.VMEM((chips, tokens, width), BF),
            pltpu.VMEM((chips, tokens, width), BF),
            pltpu.VMEM((chips, tokens, width), BF),
            pltpu.VMEM((tokens, width), BF),
            pltpu.VMEM((tokens, width), BF),
            pltpu.VMEM((shards, 1, tokens), F32),
            dma((pieces, chips)),
            dma((pieces, chips)),
            dma((pieces, chips)),
            dma((pieces, chips)),
            dma((pieces,)),
            dma((pieces,)),
            dma((shards,)),
            dma((shards,)),
        ],
        compiler_params=pltpu.CompilerParams(collective_id=4, has_side_effects=True),
    )(partial, x, gain)


def attend(grouped, new_keys, new_values, cache_keys, cache_values, lengths):
    cache_len, head_dim = cache_keys.shape[2:]
    score_scale = head_dim ** (-0.5)
    scores = (
        jnp.einsum("nkgd,nkld->nkgl", grouped, cache_keys, preferred_element_type=jnp.float32)
        * score_scale
    )
    self_score = (
        jnp.einsum("nkgd,nkd->nkg", grouped, new_keys, preferred_element_type=jnp.float32)
        * score_scale
    )
    live_mask = jnp.arange(cache_len, dtype=jnp.int32)[None, :] < lengths[:, None]
    scores = jnp.where(live_mask[:, None, None, :], scores, -1e30)
    row_top = jnp.maximum(jnp.max(scores, axis=3), self_score)
    exp_scores = jnp.exp(scores - row_top[..., None])
    self_weight = jnp.exp(self_score - row_top)
    denom_sum = jnp.sum(exp_scores, axis=3) + self_weight
    weight_bf = (exp_scores / denom_sum[..., None]).astype(jnp.bfloat16)
    self_bf = (self_weight / denom_sum).astype(jnp.bfloat16)
    context = jnp.einsum(
        "nkgl,nkld->nkgd", weight_bf, cache_values, preferred_element_type=jnp.float32
    )
    context = (
        context
        + self_bf.astype(jnp.float32)[..., None] * new_values.astype(jnp.float32)[:, :, None, :]
    )
    return context.astype(jnp.bfloat16)


def local(
    sizes,
    hidden_state,
    attn_gain,
    ffn_gain,
    w_query,
    w_keyval,
    w_output,
    cache_keys,
    cache_values,
    lengths,
):
    groups, shards = sizes
    total = groups * shards
    tokens, width = hidden_state.shape
    seqs, kv_heads, _, head_dim = cache_keys.shape
    g, s = lax.axis_index("group"), lax.axis_index("shard")
    model = width * shards
    depth = w_query.shape[0]
    q_cols, kv_cols = w_query.shape[1], w_keyval.shape[1]
    gain = lax.dynamic_slice_in_dim(attn_gain, g * depth, depth).astype(F32)[None, :]
    half_dim = head_dim // 2
    frequency = rope_base ** (-2.0 * jnp.arange(half_dim, dtype=F32) / head_dim)
    frequency = jnp.concatenate([frequency, frequency])[None, :]
    got = front(hidden_state, gain, lengths[None, :], frequency, w_query, w_keyval, sizes)
    owner_len = lax.dynamic_slice_in_dim(lengths, s * seqs, seqs)
    heads = shards * q_cols // head_dim
    fresh = got.transpose(2, 0, 1, 3).reshape(seqs, shards, q_cols + kv_cols)
    grouped = fresh[..., :q_cols].reshape(seqs, kv_heads, heads // kv_heads, head_dim)
    keyval = fresh[..., q_cols:].reshape(seqs, 2 * kv_heads, head_dim)
    new_keys, new_values = keyval[:, :kv_heads], keyval[:, kv_heads:]
    context = attend(grouped, new_keys, new_values, cache_keys, cache_values, owner_len)
    context = context.reshape(seqs, shards, q_cols).transpose(1, 0, 2)

    (rows,) = exchange(
        [context],
        [(groups, shards, seqs, q_cols)],
        sizes,
        total,
        lambda ref, pg, ps: ref.at[ps],
        lambda ref, pg, ps: ref.at[pg, ps],
        3,
    )
    partial = jnp.dot(
        rows.reshape(total * seqs, q_cols), w_output, preferred_element_type=F32
    ).astype(BF)
    ffn_scale = lax.dynamic_slice_in_dim(ffn_gain, s * width, width).astype(F32)[None, :]
    branch, ffn_input = finish(
        partial.reshape(groups, tokens, w_output.shape[1]), hidden_state, ffn_scale, sizes
    )
    return (branch, ffn_input)


def solution(mesh):
    sizes = (mesh.shape["group"], mesh.shape["shard"])
    placed = (
        P("group", "shard"),
        P(),
        P(),
        P("group", "shard"),
        P("group", "shard"),
        P("shard", "group"),
        P(("group", "shard"), None, None, None),
        P(("group", "shard"), None, None, None),
        P("group"),
    )
    return jax.shard_map(
        functools.partial(local, sizes),
        mesh=mesh,
        in_specs=placed,
        out_specs=(P("group", "shard"), P("group", "shard")),
        check_vma=False,
    )
```
